16 devices in a mesh: dp: 1, sp: 16 (over x, y, z, core).
Axes of the slice: x: 2, y: 2, z: 2, core: 2. Of those that a mesh axis runs over, the one named last changes fastest.
Arguments:
- q: bfloat16 [32, 8, 256], P('dp')
- k: bfloat16 [32, 8192, 8, 256], P('dp', 'sp')
- v: bfloat16 [32, 8192, 8, 256], P('dp', 'sp')
Outputs:
- q: bfloat16 [32, 8, 256], P('dp')
All inputs are finite; a program needn't handle non-finite values.
Results may differ from the reference program's by a relative error of at most 0.012.
Values are sent between devices in bfloat16 or wider.
A program may use at most 2 GiB of HBM per device.

```python
import jax
import jax.numpy as jnp

BATCH = 32
CACHE = 8192
HEADS = 8
KV_HEADS = 8
HEAD = 256


def setup_inputs(seed: int = 0, part: int = 0) -> dict:
    kq, kk, kv = (jax.random.fold_in(k, part) for k in jax.random.split(jax.random.key(seed), 3))
    return {
        "q": (3 * jax.random.normal(kq, (BATCH, HEADS, HEAD), jnp.float32)).astype(jnp.bfloat16),
        "k": jax.random.normal(kk, (BATCH, CACHE, KV_HEADS, HEAD), jnp.float32).astype(jnp.bfloat16),
        "v": jax.random.normal(kv, (BATCH, CACHE, KV_HEADS, HEAD), jnp.float32).astype(jnp.bfloat16),
    }


def einsum(form, a, b):
    return jnp.einsum(form, a.astype(jnp.float32), b.astype(jnp.float32))


def reference(q, k, v):
    grouped = q.reshape(BATCH, KV_HEADS, -1, HEAD)
    scores = einsum("bgsd,bugd->bgsu", grouped, k) * HEAD**-0.5
    weights = jax.nn.softmax(scores, -1).astype(jnp.bfloat16)
    return einsum("bgsu,bugd->bgsd", weights, v).astype(jnp.bfloat16).reshape(BATCH, HEADS, HEAD)
```

```python
import functools

import jax
import jax.numpy as jnp
from jax import lax
from jax.experimental import pallas as pl
from jax.experimental.pallas import tpu as pltpu
from jax.sharding import PartitionSpec as P

SLOTS = 5
LAG = 4
TAIL = 4
LOG2E = 1.4426950408889634


def tree(op, parts):
    while len(parts) > 1:
        parts = [op(*parts[i : i + 2]) if i + 1 < len(parts) else parts[i] for i in range(0, len(parts), 2)]
    return parts[0]


def attend(n, q_hbm, k_hbm, v_hbm, o_hbm, q_ref, kbuf, vbuf, scores, parts, stats, done, qsem, ksem, vsem, osem, psend, precv, ssend, srecv, dsend, drecv):
    batch, heads, head = q_ref.shape
    rows = k_hbm.shape[1]
    shared = batch - TAIL
    me = lax.axis_index("sp")

    def kcopy(b):
        slot = lax.rem(b, SLOTS)
        return pltpu.make_async_copy(k_hbm.at[b], kbuf.at[slot], ksem.at[slot])

    def vcopy(b):
        slot = lax.rem(b, SLOTS)
        return pltpu.make_async_copy(v_hbm.at[b], vbuf.at[slot], vsem.at[slot])

    def remote(ref, send, recv, peer):
        return pltpu.make_async_remote_copy(ref, ref, send, recv, device_id={"sp": peer}, device_id_type=pl.DeviceIdType.MESH)

    def part_to(b, peer):
        return (
            remote(parts.at[b, me], psend.at[b], precv.at[b], peer),
            remote(stats.at[b, me], ssend.at[b], srecv.at[b], peer),
        )

    def parts_of_others(b):
        some = pl.ds(0, n - 1)
        return (
            remote(parts.at[b, some], psend.at[b], precv.at[b], me),
            remote(stats.at[b, some], ssend.at[b], srecv.at[b], me),
        )

    def done_to(b, peer):
        return remote(done.at[b], dsend.at[b], drecv.at[b], peer)

    def done_to_others(b):
        some = pl.ds(0, n - 1)
        return remote(done.at[some], dsend.at[b], drecv.at[b], me)

    def others():
        return [lax.rem(me + j, n) for j in range(1, n)]

    lane = lax.broadcasted_iota(jnp.int32, (heads, 128), 1)
    sublane = lax.broadcasted_iota(jnp.int32, (heads, 128), 0)
    own = lax.rem(lane, heads) == sublane

    def turn(b, first=False, last=False):
        tiles = rows // 256
        if not first:
            high = tree(jnp.maximum, [jnp.where(own, scores[:, pl.ds(128 * i, 128)], -jnp.inf) for i in range(rows // 128)])
            high = jnp.max(high, -1, keepdims=True)
            weights = [jnp.exp2(jnp.where(own, (scores[:, pl.ds(128 * i, 128)] - high) * (head**-0.5 * LOG2E), -jnp.inf)) for i in range(rows // 128)]
            total = jnp.sum(tree(jnp.add, weights), -1, keepdims=True)
            weights = [w.astype(jnp.bfloat16) for w in weights]
        seen = None
        slot, vslot = lax.rem(b, SLOTS), lax.rem(b + SLOTS - 1, SLOTS)
        kept = []
        for t in range(tiles + LAG):
            if t < tiles and not last:
                kept.append(lax.dot_general(q_ref[b], kbuf[slot, pl.ds(256 * t, 256)], (((1,), (1,)), ((), ())), preferred_element_type=jnp.float32))
            if t >= LAG and not first:
                u = t - LAG
                w = jnp.concatenate([weights[2 * u], weights[2 * u + 1]], -1)
                d = jnp.dot(w, vbuf[vslot, pl.ds(256 * u, 256)], preferred_element_type=jnp.float32)
                seen = d if seen is None else seen + d
        for t, s in enumerate(kept):
            scores[:, pl.ds(256 * t, 256)] = s
        if not first:
            parts[b - 1, me] = seen.astype(jnp.bfloat16)
            row = jnp.where(lane == sublane, high * head**-0.5, 0.0) + jnp.where(lane == sublane + heads, total, 0.0)
            stats[b - 1, me] = jnp.sum(row, 0, keepdims=True)

    def combine(b):
        high, total = [], []
        for i in range(n):
            row = jnp.broadcast_to(stats[b, i], (heads, 128))
            high.append(jnp.sum(jnp.where(lane == sublane, row, 0.0), -1, keepdims=True))
            total.append(jnp.sum(jnp.where(lane == sublane + heads, row, 0.0), -1, keepdims=True))
        top = tree(jnp.maximum, high)
        scale = [jnp.exp(h - top) for h in high]
        total = tree(jnp.add, [t * s for t, s in zip(total, scale)])
        seen = tree(jnp.add, [parts[b, i].astype(jnp.float32) * s for i, s in enumerate(scale)])
        done[b] = (seen / total).astype(jnp.bfloat16)

    def send(b):
        owner = lax.rem(b, n)

        @pl.when(me != owner)
        def _():
            for copy in part_to(b, owner):
                copy.start()

    def own_up(b):
        owner = lax.rem(b, n)

        @pl.when(me == owner)
        def _():
            for copy in parts_of_others(b):
                copy.wait_recv()
            combine(b)
            for peer in others():
                done_to(b, peer).start()

        @pl.when(me != owner)
        def _():
            for copy in part_to(b, owner):
                copy.wait_send()

    def settle(b):
        owner = lax.rem(b, n)

        @pl.when(me == owner)
        def _():
            done_to_others(b).wait_send()

        @pl.when(me != owner)
        def _():
            done_to(b, owner).wait_recv()

    def send_all(b):
        for peer in others():
            for copy in part_to(b, peer):
                copy.start()

    def gather(b):
        for copy in parts_of_others(b):
            copy.wait_recv()
        combine(b)

    qcopy = pltpu.make_async_copy(q_hbm, q_ref, qsem)
    qcopy.start()
    for b in range(SLOTS):
        kcopy(b).start()
        vcopy(b).start()

    barrier = pltpu.get_barrier_semaphore()
    for peer in others():
        pl.semaphore_signal(barrier, 1, device_id={"sp": peer}, device_id_type=pl.DeviceIdType.MESH)
    pl.semaphore_wait(barrier, n - 1)

    qcopy.wait()
    kcopy(0).wait()
    turn(0, first=True)

    def body(b, _):
        @pl.when(b + SLOTS - 1 < batch)
        def _():
            kcopy(b + SLOTS - 1).start()

        @pl.when(b >= 2)
        def _():
            send(b - 2)

        @pl.when(b >= 4)
        def _():
            own_up(b - 4)

        @pl.when(b >= 8)
        def _():
            settle(b - 8)

        kcopy(b).wait()
        vcopy(b - 1).wait()
        turn(b)

        @pl.when(b + SLOTS - 1 < batch)
        def _():
            vcopy(b + SLOTS - 1).start()

    lax.fori_loop(1, shared + 1, body, None)
    for b in range(shared + 1, batch + 1):
        if b - 2 < shared:
            send(b - 2)
        else:
            send_all(b - 2)
        if b - 4 < shared:
            own_up(b - 4)
        if b - 8 < shared:
            settle(b - 8)
        if b < batch:
            kcopy(b).wait()
        vcopy(b - 1).wait()
        turn(b, last=b == batch)
    send_all(batch - 1)
    for b in range(batch - 3, shared):
        own_up(b)
    for b in range(shared, batch - 1):
        gather(b)
    for b in range(batch - 7, shared):
        settle(b)
    early = pltpu.make_async_copy(done.at[pl.ds(0, batch - 1)], o_hbm.at[pl.ds(0, batch - 1)], osem.at[0])
    early.start()
    gather(batch - 1)
    late = pltpu.make_async_copy(done.at[pl.ds(batch - 1, 1)], o_hbm.at[pl.ds(batch - 1, 1)], osem.at[1])
    late.start()
    for b in range(shared, batch):
        for copy in parts_of_others(b):
            copy.wait_send()
    early.wait()
    late.wait()


def solution(mesh):
    n = mesh.shape["sp"]

    def step(q, k, v):
        batch, tokens, heads, head = k.shape
        rows = tokens * heads
        return pl.pallas_call(
            functools.partial(attend, n),
            out_shape=jax.ShapeDtypeStruct(q.shape, q.dtype),
            in_specs=[pl.BlockSpec(memory_space=pl.ANY)] * 3,
            out_specs=pl.BlockSpec(memory_space=pl.ANY),
            scratch_shapes=[
                pltpu.VMEM((batch, heads, head), jnp.bfloat16),
                pltpu.VMEM((SLOTS, rows, head), jnp.bfloat16),
                pltpu.VMEM((SLOTS, rows, head), jnp.bfloat16),
                pltpu.VMEM((heads, rows), jnp.float32),
                pltpu.VMEM((batch, n, heads, head), jnp.bfloat16),
                pltpu.VMEM((batch, n, 1, 128), jnp.float32),
                pltpu.VMEM((batch, heads, head), jnp.bfloat16),
                pltpu.SemaphoreType.DMA,
                pltpu.SemaphoreType.DMA((SLOTS,)),
                pltpu.SemaphoreType.DMA((SLOTS,)),
                pltpu.SemaphoreType.DMA((2,)),
                *[pltpu.SemaphoreType.DMA((batch,))] * 6,
            ],
            compiler_params=pltpu.CompilerParams(vmem_limit_bytes=56 * 2**20, collective_id=0, has_side_effects=True),
        )(q, k.reshape(batch, rows, head), v.reshape(batch, rows, head))

    return jax.shard_map(
        step,
        mesh=mesh,
        in_specs=(P("dp", None, None), P("dp", "sp", None, None), P("dp", "sp", None, None)),
        out_specs=P("dp", None, None),
        check_vma=False,
    )
```

```python
import functools

import jax
import jax.numpy as jnp
from jax import lax
from jax.experimental import pallas as pl
from jax.experimental.pallas import tpu as pltpu
from jax.sharding import PartitionSpec as P

SLOTS = 5
LAG = 4
WAIT = 6
TAIL = 6
LOG2E = 1.4426950408889634


def tree(op, parts):
    while len(parts) > 1:
        parts = [op(*parts[i : i + 2]) if i + 1 < len(parts) else parts[i] for i in range(0, len(parts), 2)]
    return parts[0]


def attend(n, q_hbm, k_hbm, v_hbm, done, q_ref, kbuf, vbuf, scores, parts, stats, qsem, ksem, vsem, psend, ssend, dsend, drecv, precv, srecv):
    batch, heads, head = q_ref.shape
    rows = k_hbm.shape[1]
    shared = batch - TAIL
    me = lax.axis_index("sp")

    def kcopy(b):
        slot = lax.rem(b, SLOTS)
        return pltpu.make_async_copy(k_hbm.at[b], kbuf.at[slot], ksem.at[slot])

    def vcopy(b):
        slot = lax.rem(b, SLOTS)
        return pltpu.make_async_copy(v_hbm.at[b], vbuf.at[slot], vsem.at[slot])

    def remote(ref, send, recv, peer):
        return pltpu.make_async_remote_copy(ref, ref, send, recv, device_id={"sp": peer}, device_id_type=pl.DeviceIdType.MESH)

    def others():
        return [lax.rem(me + j, n) for j in range(1, n)]

    def send_part(b, sem, peer):
        remote(parts.at[b, me], psend, precv.at[sem], peer).start()
        remote(stats.at[b, me], ssend, srecv.at[sem], peer).start()

    lane = lax.broadcasted_iota(jnp.int32, (heads, 128), 1)
    sublane = lax.broadcasted_iota(jnp.int32, (heads, 128), 0)
    own = lax.rem(lane, heads) == sublane

    def turn(b, first=False, last=False):
        tiles = rows // 256
        if not first:
            high = tree(jnp.maximum, [jnp.where(own, scores[:, pl.ds(128 * i, 128)], -jnp.inf) for i in range(rows // 128)])
            high = jnp.max(high, -1, keepdims=True)
            weights = [jnp.exp2(jnp.where(own, (scores[:, pl.ds(128 * i, 128)] - high) * (head**-0.5 * LOG2E), -jnp.inf)) for i in range(rows // 128)]
            total = jnp.sum(tree(jnp.add, weights), -1, keepdims=True)
            weights = [w.astype(jnp.bfloat16) for w in weights]
        seen = None
        slot, vslot = lax.rem(b, SLOTS), lax.rem(b + SLOTS - 1, SLOTS)
        kept = []
        for t in range(tiles + LAG):
            if t < tiles and not last:
                kept.append(lax.dot_general(q_ref[b], kbuf[slot, pl.ds(256 * t, 256)], (((1,), (1,)), ((), ())), preferred_element_type=jnp.float32))
            if t >= LAG and not first:
                u = t - LAG
                w = jnp.concatenate([weights[2 * u], weights[2 * u + 1]], -1)
                d = jnp.dot(w, vbuf[vslot, pl.ds(256 * u, 256)], preferred_element_type=jnp.float32)
                seen = d if seen is None else seen + d
        for t, s in enumerate(kept):
            scores[:, pl.ds(256 * t, 256)] = s
        if not first:
            parts[b - 1, me] = seen.astype(jnp.bfloat16)
            row = jnp.where(lane == sublane, high * head**-0.5, 0.0) + jnp.where(lane == sublane + heads, total, 0.0)
            stats[b - 1, me] = jnp.sum(row, 0, keepdims=True)

    def gather(b, sem):
        some = pl.ds(0, n - 1)
        remote(parts.at[b, some], psend, precv.at[sem], me).wait_recv()
        remote(stats.at[b, some], ssend, srecv.at[sem], me).wait_recv()
        high, total = [], []
        for i in range(n):
            row = jnp.broadcast_to(stats[b, i], (heads, 128))
            high.append(jnp.sum(jnp.where(lane == sublane, row, 0.0), -1, keepdims=True))
            total.append(jnp.sum(jnp.where(lane == sublane + heads, row, 0.0), -1, keepdims=True))
        top = tree(jnp.maximum, high)
        scale = [jnp.exp(h - top) for h in high]
        total = tree(jnp.add, [t * s for t, s in zip(total, scale)])
        seen = tree(jnp.add, [parts[b, i].astype(jnp.float32) * s for i, s in enumerate(scale)])
        done[b] = (seen / total).astype(jnp.bfloat16)

    def send(b):
        owner = lax.rem(b, n)

        @pl.when(me != owner)
        def _():
            send_part(b, b // n, owner)

    def own_up(b):
        @pl.when(me == lax.rem(b, n))
        def _():
            gather(b, b // n)
            for peer in others():
                remote(done.at[b], dsend, drecv, peer).start()

    def send_all(b):
        for peer in others():
            send_part(b, b - shared + pl.cdiv(shared, n), peer)

    qcopy = pltpu.make_async_copy(q_hbm, q_ref, qsem)
    qcopy.start()
    for b in range(SLOTS):
        kcopy(b).start()
        vcopy(b).start()

    barrier = pltpu.get_barrier_semaphore()
    for peer in others():
        pl.semaphore_signal(barrier, 1, device_id={"sp": peer}, device_id_type=pl.DeviceIdType.MESH)
    pl.semaphore_wait(barrier, n - 1)

    qcopy.wait()
    kcopy(0).wait()
    turn(0, first=True)

    def body(b, _):
        @pl.when(b + SLOTS - 1 < batch)
        def _():
            kcopy(b + SLOTS - 1).start()

        @pl.when((b >= 2) & (b - 2 < shared))
        def _():
            send(b - 2)

        @pl.when(b - 2 >= shared)
        def _():
            send_all(b - 2)

        @pl.when((b >= WAIT) & (b - WAIT < shared))
        def _():
            own_up(b - WAIT)

        kcopy(b).wait()
        vcopy(b - 1).wait()
        turn(b)

        @pl.when(b + SLOTS - 1 < batch)
        def _():
            vcopy(b + SLOTS - 1).start()

    lax.fori_loop(1, batch, body, None)
    send_all(batch - 2)
    vcopy(batch - 1).wait()
    turn(batch, last=True)
    send_all(batch - 1)
    for b in range(batch - WAIT, shared):
        own_up(b)
    for b in range(shared, batch):
        gather(b, b - shared + pl.cdiv(shared, n))

    for mine in {shared // n, pl.cdiv(shared, n)}:
        sent = shared - mine

        @pl.when((me < shared % n) == (mine > shared // n))
        def _():
            remote(done.at[pl.ds(0, sent)], dsend, drecv, me).wait_recv()
            for _ in range(mine):
                remote(done.at[pl.ds(0, n - 1)], dsend, drecv, me).wait_send()
            remote(parts.at[pl.ds(0, sent), 0], psend, precv.at[0], me).wait_send()
            remote(stats.at[pl.ds(0, sent), 0], ssend, srecv.at[0], me).wait_send()

    remote(parts.at[pl.ds(0, TAIL), pl.ds(0, n - 1)], psend, precv.at[0], me).wait_send()
    remote(stats.at[pl.ds(0, TAIL), pl.ds(0, n - 1)], ssend, srecv.at[0], me).wait_send()


def solution(mesh):
    n = mesh.shape["sp"]

    def step(q, k, v):
        batch, tokens, heads, head = k.shape
        rows = tokens * heads
        return pl.pallas_call(
            functools.partial(attend, n),
            out_shape=jax.ShapeDtypeStruct(q.shape, q.dtype),
            in_specs=[pl.BlockSpec(memory_space=pl.ANY)] * 3,
            out_specs=pl.BlockSpec(memory_space=pltpu.VMEM),
            scratch_shapes=[
                pltpu.VMEM((batch, heads, head), jnp.bfloat16),
                pltpu.VMEM((SLOTS, rows, head), jnp.bfloat16),
                pltpu.VMEM((SLOTS, rows, head), jnp.bfloat16),
                pltpu.VMEM((heads, rows), jnp.float32),
                pltpu.VMEM((batch, n, heads, head), jnp.bfloat16),
                pltpu.VMEM((batch, n, 1, 128), jnp.float32),
                pltpu.SemaphoreType.DMA,
                pltpu.SemaphoreType.DMA((SLOTS,)),
                pltpu.SemaphoreType.DMA((SLOTS,)),
                *[pltpu.SemaphoreType.DMA] * 4,
                *[pltpu.SemaphoreType.DMA((pl.cdiv(batch - TAIL, n) + TAIL,))] * 2,
            ],
            compiler_params=pltpu.CompilerParams(vmem_limit_bytes=215 * 2**18, collective_id=0, has_side_effects=True),
        )(q, k.reshape(batch, rows, head), v.reshape(batch, rows, head))

    return jax.shard_map(
        step,
        mesh=mesh,
        in_specs=(P("dp", None, None), P("dp", "sp", None, None), P("dp", "sp", None, None)),
        out_specs=P("dp", None, None),
        check_vma=False,
    )
```

```python
import functools

import jax
import jax.numpy as jnp
from jax import lax
from jax.experimental import pallas as pl
from jax.experimental.pallas import tpu as pltpu
from jax.sharding import PartitionSpec as P

SLOTS = 5
LAG = 4
WAIT = 6
TAIL = 8
LOG2E = 1.4426950408889634


def tree(op, parts):
    while len(parts) > 1:
        parts = [op(*parts[i : i + 2]) if i + 1 < len(parts) else parts[i] for i in range(0, len(parts), 2)]
    return parts[0]


def attend(n, q_hbm, k_hbm, v_hbm, done, q_ref, kbuf, vbuf, scores, parts, stats, qsem, ksem, vsem, psend, ssend, dsend, drecv, precv, srecv):
    batch, heads, head = q_ref.shape
    rows = k_hbm.shape[1]
    shared = batch - TAIL
    me = lax.axis_index("sp")

    def kcopy(b):
        slot = lax.rem(b, SLOTS)
        return pltpu.make_async_copy(k_hbm.at[b], kbuf.at[slot], ksem.at[slot])

    def vcopy(b):
        slot = lax.rem(b, SLOTS)
        return pltpu.make_async_copy(v_hbm.at[b], vbuf.at[slot], vsem.at[slot])

    def remote(ref, send, recv, peer):
        return pltpu.make_async_remote_copy(ref, ref, send, recv, device_id={"sp": peer}, device_id_type=pl.DeviceIdType.MESH)

    peers = [j + lax.div(n + j - me, n) for j in range(n - 1)]

    def send_part(b, sem, peer):
        remote(parts.at[b, me], psend, precv.at[sem], peer).start()
        remote(stats.at[b, me], ssend, srecv.at[sem], peer).start()

    lane = lax.broadcasted_iota(jnp.int32, (heads, 128), 1)
    sublane = lax.broadcasted_iota(jnp.int32, (heads, 128), 0)
    own = lax.rem(lane, heads) == sublane

    tiles = rows // 256

    def scale_rows():
        high = tree(jnp.maximum, [jnp.where(own, scores[:, pl.ds(128 * i, 128)], -jnp.inf) for i in range(rows // 128)])
        high = jnp.max(high, -1, keepdims=True)
        weights = [jnp.exp2(jnp.where(own, (scores[:, pl.ds(128 * i, 128)] - high) * (head**-0.5 * LOG2E), -jnp.inf)) for i in range(rows // 128)]
        total = jnp.sum(tree(jnp.add, weights), -1, keepdims=True)
        weights = [jnp.concatenate([w.astype(jnp.bfloat16) for w in weights[i : i + 2]], -1) for i in range(0, len(weights), 2)]
        return weights, total, high

    def score(b, t):
        return lax.dot_general(q_ref[b], kbuf[lax.rem(b, SLOTS), pl.ds(256 * t, 256)], (((1,), (1,)), ((), ())), preferred_element_type=jnp.float32)

    def value(b, t, weights):
        return jnp.dot(weights[t], vbuf[lax.rem(b, SLOTS), pl.ds(256 * t, 256)], preferred_element_type=jnp.float32)

    def keep(found):
        for t, s in enumerate(found):
            scores[:, pl.ds(256 * t, 256)] = s

    def part(b, seen, total, high):
        parts[b, me] = seen.astype(jnp.bfloat16)
        row = jnp.where(lane == sublane, high * head**-0.5, 0.0) + jnp.where(lane == sublane + heads, total, 0.0)
        stats[b, me] = jnp.sum(row, 0, keepdims=True)

    def turn(b):
        weights, total, high = scale_rows()
        found, seen = [], []
        for t in range(tiles + LAG):
            if t < tiles:
                found.append(score(b, t))
            if t >= LAG:
                seen.append(value(b - 1, t - LAG, weights))
        keep(found)
        part(b - 1, functools.reduce(jnp.add, seen), total, high)

    def gather(b, sem):
        some = pl.ds(0, n - 1)
        remote(parts.at[b, some], psend, precv.at[sem], me).wait_recv()
        remote(stats.at[b, some], ssend, srecv.at[sem], me).wait_recv()
        high, total = [], []
        for i in range(n):
            row = jnp.broadcast_to(stats[b, i], (heads, 128))
            high.append(jnp.sum(jnp.where(lane == sublane, row, 0.0), -1, keepdims=True))
            total.append(jnp.sum(jnp.where(lane == sublane + heads, row, 0.0), -1, keepdims=True))
        top = tree(jnp.maximum, high)
        scale = [jnp.exp(h - top) for h in high]
        total = tree(jnp.add, [t * s for t, s in zip(total, scale)])
        seen = tree(jnp.add, [parts[b, i].astype(jnp.float32) * s for i, s in enumerate(scale)])
        done[b] = (seen / total).astype(jnp.bfloat16)

    def send(b):
        owner = lax.rem(b, n)

        @pl.when(me != owner)
        def _():
            send_part(b, b // n, owner)

    def own_up(b):
        @pl.when(me == lax.rem(b, n))
        def _():
            gather(b, b // n)
            for peer in peers:
                remote(done.at[b], dsend, drecv, peer).start()

    def send_all(b, some=slice(None)):
        for peer in peers[some]:
            send_part(b, b - shared + pl.cdiv(shared, n), peer)

    qcopy = pltpu.make_async_copy(q_hbm, q_ref, qsem)
    qcopy.start()
    kcopy(0).start()
    for b in range(1, SLOTS):
        kcopy(b).start()
        vcopy(b - 1).start()

    barrier = pltpu.get_barrier_semaphore()
    for peer in peers:
        pl.semaphore_signal(barrier, 1, device_id={"sp": peer}, device_id_type=pl.DeviceIdType.MESH)
    pl.semaphore_wait(barrier, n - 1)

    qcopy.wait()
    kcopy(0).wait()
    keep([score(0, t) for t in range(tiles)])
    kcopy(SLOTS).start()
    vcopy(SLOTS - 1).start()

    def body(b, _):
        @pl.when((b >= 2) & (b - 2 < shared))
        def _():
            send(b - 2)

        @pl.when(b - 2 >= shared)
        def _():
            send_all(b - 2)

        @pl.when((b >= WAIT) & (b - WAIT < shared))
        def _():
            own_up(b - WAIT)

        kcopy(b).wait()
        vcopy(b - 1).wait()
        turn(b)

        @pl.when(b + SLOTS < batch)
        def _():
            kcopy(b + SLOTS).start()

        @pl.when(b + SLOTS - 1 < batch)
        def _():
            vcopy(b + SLOTS - 1).start()

    lax.fori_loop(1, batch, body, None)
    weights, total, high = scale_rows()
    send_all(batch - 2, slice(2))
    vcopy(batch - 1).wait()
    seen = [value(batch - 1, t, weights) for t in range(tiles)]
    one, other = functools.reduce(jnp.add, seen[::2]), functools.reduce(jnp.add, seen[1::2])
    part(batch - 1, one + jnp.where(me >= 0, other, 0.0), total, high)
    send_all(batch - 1)
    send_all(batch - 2, slice(2, None))
    for b in range(batch - WAIT, shared):
        own_up(b)

    def last(b, _):
        gather(b, b - shared + pl.cdiv(shared, n))

    lax.fori_loop(shared, batch, last, None)

    for mine in {shared // n, pl.cdiv(shared, n)}:
        sent = shared - mine

        @pl.when((me < shared % n) == (mine > shared // n))
        def _():
            remote(done.at[pl.ds(0, sent)], dsend, drecv, me).wait_recv()
            for _ in range(mine):
                remote(done.at[pl.ds(0, n - 1)], dsend, drecv, me).wait_send()
            remote(parts.at[pl.ds(0, sent), 0], psend, precv.at[0], me).wait_send()
            remote(stats.at[pl.ds(0, sent), 0], ssend, srecv.at[0], me).wait_send()

    remote(parts.at[pl.ds(0, TAIL), pl.ds(0, n - 1)], psend, precv.at[0], me).wait_send()
    remote(stats.at[pl.ds(0, TAIL), pl.ds(0, n - 1)], ssend, srecv.at[0], me).wait_send()


def solution(mesh):
    n = mesh.shape["sp"]

    def step(q, k, v):
        batch, tokens, heads, head = k.shape
        rows = tokens * heads
        return pl.pallas_call(
            functools.partial(attend, n),
            out_shape=jax.ShapeDtypeStruct(q.shape, q.dtype),
            in_specs=[pl.BlockSpec(memory_space=pl.ANY)] * 3,
            out_specs=pl.BlockSpec(memory_space=pltpu.VMEM),
            scratch_shapes=[
                pltpu.VMEM((batch, heads, head), jnp.bfloat16),
                pltpu.VMEM((SLOTS, rows, head), jnp.bfloat16),
                pltpu.VMEM((SLOTS, rows, head), jnp.bfloat16),
                pltpu.VMEM((heads, rows), jnp.float32),
                pltpu.VMEM((batch, n, heads, head), jnp.bfloat16),
                pltpu.VMEM((batch, n, 1, 128), jnp.float32),
                pltpu.SemaphoreType.DMA,
                pltpu.SemaphoreType.DMA((SLOTS,)),
                pltpu.SemaphoreType.DMA((SLOTS,)),
                *[pltpu.SemaphoreType.DMA] * 4,
                *[pltpu.SemaphoreType.DMA((pl.cdiv(batch - TAIL, n) + TAIL,))] * 2,
            ],
            compiler_params=pltpu.CompilerParams(vmem_limit_bytes=215 * 2**18, collective_id=0, has_side_effects=True),
        )(q, k.reshape(batch, rows, head), v.reshape(batch, rows, head))

    return jax.shard_map(
        step,
        mesh=mesh,
        in_specs=(P("dp", None, None), P("dp", "sp", None, None), P("dp", "sp", None, None)),
        out_specs=P("dp", None, None),
        check_vma=False,
    )
```

```python
import functools

import jax
import jax.numpy as jnp
from jax import lax
from jax.experimental import pallas as pl
from jax.experimental.pallas import tpu as pltpu
from jax.sharding import PartitionSpec as P

SLOTS = 5
LEAD = 2
LAG = 4
WAIT = 7
TAIL = 6
LOG2E = 1.4426950408889634


def tree(op, parts):
    while len(parts) > 1:
        parts = [op(*parts[i : i + 2]) if i + 1 < len(parts) else parts[i] for i in range(0, len(parts), 2)]
    return parts[0]


def attend(n, q_hbm, k_hbm, v_hbm, done, q_ref, kbuf, vbuf, scores, parts, stats, qsem, ksem, vsem, psend, ssend, dsend, drecv, precv, srecv):
    batch, heads, head = q_ref.shape
    rows = k_hbm.shape[1]
    shared = batch - TAIL
    me = lax.axis_index("sp")

    def kcopy(b):
        slot = lax.rem(b, SLOTS)
        return pltpu.make_async_copy(k_hbm.at[b], kbuf.at[slot], ksem.at[slot])

    def vcopy(b):
        slot = lax.rem(b, SLOTS)
        return pltpu.make_async_copy(v_hbm.at[b], vbuf.at[slot], vsem.at[slot])

    def remote(ref, send, recv, peer):
        return pltpu.make_async_remote_copy(ref, ref, send, recv, device_id={"sp": peer}, device_id_type=pl.DeviceIdType.MESH)

    peers = [j + lax.div(n + j - me, n) for j in range(n - 1)]

    def send_part(b, sem, peer):
        remote(parts.at[b, me], psend, precv.at[sem], peer).start()
        remote(stats.at[b, me], ssend, srecv.at[sem], peer).start()

    lane = lax.broadcasted_iota(jnp.int32, (heads, 128), 1)
    sublane = lax.broadcasted_iota(jnp.int32, (heads, 128), 0)
    own = lax.rem(lane, heads) == sublane

    tiles = rows // 256

    def scale_rows(b):
        row = scores.at[lax.rem(b, LEAD + 1)]
        high = tree(jnp.maximum, [jnp.where(own, row[:, pl.ds(128 * i, 128)], -jnp.inf) for i in range(rows // 128)])
        high = jnp.max(high, -1, keepdims=True)
        weights = [jnp.exp2(jnp.where(own, (row[:, pl.ds(128 * i, 128)] - high) * (head**-0.5 * LOG2E), -jnp.inf)) for i in range(rows // 128)]
        total = jnp.sum(tree(jnp.add, weights), -1, keepdims=True)
        weights = [jnp.concatenate([w.astype(jnp.bfloat16) for w in weights[i : i + 2]], -1) for i in range(0, len(weights), 2)]
        return weights, total, high

    def score(b, t):
        return lax.dot_general(q_ref[b], kbuf[lax.rem(b, SLOTS), pl.ds(256 * t, 256)], (((1,), (1,)), ((), ())), preferred_element_type=jnp.float32)

    def value(b, t, weights):
        return jnp.dot(weights[t], vbuf[lax.rem(b, SLOTS), pl.ds(256 * t, 256)], preferred_element_type=jnp.float32)

    def keep(b, found):
        for t, s in enumerate(found):
            scores[lax.rem(b, LEAD + 1), :, pl.ds(256 * t, 256)] = s

    def part(b, seen, total, high):
        parts[b, me] = seen.astype(jnp.bfloat16)
        row = jnp.where(lane == sublane, high * head**-0.5, 0.0) + jnp.where(lane == sublane + heads, total, 0.0)
        stats[b, me] = jnp.sum(row, 0, keepdims=True)

    def turn(b):
        weights, total, high = scale_rows(b - LEAD)
        found, seen = [], []
        for t in range(tiles + LAG):
            if t < tiles:
                found.append(score(b, t))
            if t >= LAG:
                seen.append(value(b - LEAD, t - LAG, weights))
        keep(b, found)
        part(b - LEAD, functools.reduce(jnp.add, seen), total, high)

    def values(b, weights):
        seen = [value(b, t, weights) for t in range(tiles)]
        one, other = functools.reduce(jnp.add, seen[::2]), functools.reduce(jnp.add, seen[1::2])
        return one + jnp.where(me >= 0, other, 0.0)

    def gather(b, sem):
        some = pl.ds(0, n - 1)
        remote(parts.at[b, some], psend, precv.at[sem], me).wait_recv()
        remote(stats.at[b, some], ssend, srecv.at[sem], me).wait_recv()
        high, total = [], []
        for i in range(n):
            row = jnp.broadcast_to(stats[b, i], (heads, 128))
            high.append(jnp.sum(jnp.where(lane == sublane, row, 0.0), -1, keepdims=True))
            total.append(jnp.sum(jnp.where(lane == sublane + heads, row, 0.0), -1, keepdims=True))
        top = tree(jnp.maximum, high)
        scale = [jnp.exp(h - top) for h in high]
        total = tree(jnp.add, [t * s for t, s in zip(total, scale)])
        seen = tree(jnp.add, [parts[b, i].astype(jnp.float32) * s for i, s in enumerate(scale)])
        done[b] = (seen / total).astype(jnp.bfloat16)

    def send(b):
        owner = lax.rem(b, n)

        @pl.when(me != owner)
        def _():
            send_part(b, b // n, owner)

    def own_up(b):
        @pl.when(me == lax.rem(b, n))
        def _():
            gather(b, b // n)
            for peer in peers:
                remote(done.at[b], dsend, drecv, peer).start()

    def send_all(b, some=slice(None)):
        for peer in peers[some]:
            send_part(b, b - shared + pl.cdiv(shared, n), peer)

    qcopy = pltpu.make_async_copy(q_hbm, q_ref, qsem)
    qcopy.start()
    for b in range(SLOTS):
        kcopy(b).start()
        if b >= LEAD:
            vcopy(b - LEAD).start()

    barrier = pltpu.get_barrier_semaphore()
    for peer in peers:
        pl.semaphore_signal(barrier, 1, device_id={"sp": peer}, device_id_type=pl.DeviceIdType.MESH)
    pl.semaphore_wait(barrier, n - 1)

    qcopy.wait()
    for b in range(LEAD):
        kcopy(b).wait()
        keep(b, [score(b, t) for t in range(tiles)])
        kcopy(b + SLOTS).start()
        vcopy(b + SLOTS - LEAD).start()

    def body(b, _):
        @pl.when((b > LEAD) & (b - LEAD - 1 < shared))
        def _():
            send(b - LEAD - 1)

        @pl.when(b - LEAD - 1 >= shared)
        def _():
            send_all(b - LEAD - 1)

        @pl.when((b >= WAIT) & (b - WAIT < shared))
        def _():
            own_up(b - WAIT)

        kcopy(b).wait()
        vcopy(b - LEAD).wait()
        turn(b)

        @pl.when(b + SLOTS < batch)
        def _():
            kcopy(b + SLOTS).start()

        @pl.when(b + SLOTS - LEAD < batch)
        def _():
            vcopy(b + SLOTS - LEAD).start()

    lax.fori_loop(LEAD, batch, body, None)
    ready = scale_rows(batch - LEAD)
    for b in range(batch - LEAD, batch):
        send_all(b - 1, slice(2))
        vcopy(b).wait()
        weights, total, high = ready
        if b + 1 < batch:
            ready = scale_rows(b + 1)
        part(b, values(b, weights), total, high)
    send_all(batch - 1)
    for b in range(batch - 2, batch - LEAD - 2, -1):
        send_all(b, slice(2, None))
    for b in range(batch - WAIT, shared):
        own_up(b)

    def last(b, _):
        gather(b, b - shared + pl.cdiv(shared, n))

    lax.fori_loop(shared, batch, last, None)

    for mine in {shared // n, pl.cdiv(shared, n)}:
        sent = shared - mine

        @pl.when((me < shared % n) == (mine > shared // n))
        def _():
            remote(done.at[pl.ds(0, sent)], dsend, drecv, me).wait_recv()
            for _ in range(mine):
                remote(done.at[pl.ds(0, n - 1)], dsend, drecv, me).wait_send()
            remote(parts.at[pl.ds(0, sent), 0], psend, precv.at[0], me).wait_send()
            remote(stats.at[pl.ds(0, sent), 0], ssend, srecv.at[0], me).wait_send()

    remote(parts.at[pl.ds(0, TAIL), pl.ds(0, n - 1)], psend, precv.at[0], me).wait_send()
    remote(stats.at[pl.ds(0, TAIL), pl.ds(0, n - 1)], ssend, srecv.at[0], me).wait_send()


def solution(mesh):
    n = mesh.shape["sp"]

    def step(q, k, v):
        batch, tokens, heads, head = k.shape
        rows = tokens * heads
        return pl.pallas_call(
            functools.partial(attend, n),
            out_shape=jax.ShapeDtypeStruct(q.shape, q.dtype),
            in_specs=[pl.BlockSpec(memory_space=pl.ANY)] * 3,
            out_specs=pl.BlockSpec(memory_space=pltpu.VMEM),
            scratch_shapes=[
                pltpu.VMEM((batch, heads, head), jnp.bfloat16),
                pltpu.VMEM((SLOTS, rows, head), jnp.bfloat16),
                pltpu.VMEM((SLOTS, rows, head), jnp.bfloat16),
                pltpu.VMEM((LEAD + 1, heads, rows), jnp.float32),
                pltpu.VMEM((batch, n, heads, head), jnp.bfloat16),
                pltpu.VMEM((batch, n, 1, 128), jnp.float32),
                pltpu.SemaphoreType.DMA,
                pltpu.SemaphoreType.DMA((SLOTS,)),
                pltpu.SemaphoreType.DMA((SLOTS,)),
                *[pltpu.SemaphoreType.DMA] * 4,
                *[pltpu.SemaphoreType.DMA((pl.cdiv(batch - TAIL, n) + TAIL,))] * 2,
            ],
            compiler_params=pltpu.CompilerParams(vmem_limit_bytes=215 * 2**18, collective_id=0, has_side_effects=True),
        )(q, k.reshape(batch, rows, head), v.reshape(batch, rows, head))

    return jax.shard_map(
        step,
        mesh=mesh,
        in_specs=(P("dp", None, None), P("dp", "sp", None, None), P("dp", "sp", None, None)),
        out_specs=P("dp", None, None),
        check_vma=False,
    )
```

```python
import functools

import jax
import jax.numpy as jnp
from jax import lax
from jax.experimental import pallas as pl
from jax.experimental.pallas import tpu as pltpu
from jax.sharding import PartitionSpec as P

SLOTS = 4
LEAD = 2
LAG = 4
WAIT = 7
TAIL = 6
LOG2E = 1.4426950408889634


def tree(op, parts):
    while len(parts) > 1:
        parts = [op(*parts[i : i + 2]) if i + 1 < len(parts) else parts[i] for i in range(0, len(parts), 2)]
    return parts[0]


def attend(n, q_hbm, k_hbm, v_hbm, done, q_ref, kbuf, vbuf, scores, parts, stats, qsem, ksem, vsem, psend, ssend, dsend, drecv, precv, srecv):
    batch, heads, head = q_ref.shape
    rows = k_hbm.shape[1]
    shared = batch - TAIL
    me = lax.axis_index("sp")

    def kcopy(b):
        slot = lax.rem(b, SLOTS)
        return pltpu.make_async_copy(k_hbm.at[b], kbuf.at[slot], ksem.at[slot])

    def vcopy(b):
        slot = lax.rem(b, SLOTS)
        return pltpu.make_async_copy(v_hbm.at[b], vbuf.at[slot], vsem.at[slot])

    def remote(ref, send, recv, peer):
        return pltpu.make_async_remote_copy(ref, ref, send, recv, device_id={"sp": peer}, device_id_type=pl.DeviceIdType.MESH)

    peers = [j + lax.div(n + j - me, n) for j in range(n - 1)]

    def send_part(b, sem, peer):
        remote(parts.at[b, me], psend, precv.at[sem], peer).start()
        remote(stats.at[b, me], ssend, srecv.at[sem], peer).start()

    lane = lax.broadcasted_iota(jnp.int32, (heads, 128), 1)
    sublane = lax.broadcasted_iota(jnp.int32, (heads, 128), 0)
    own = lax.rem(lane, heads) == sublane

    tiles = rows // 256

    def scale_rows(b):
        row = scores.at[lax.rem(b, LEAD + 1)]
        high = tree(jnp.maximum, [jnp.where(own, row[:, pl.ds(128 * i, 128)], -jnp.inf) for i in range(rows // 128)])
        high = jnp.max(high, -1, keepdims=True)
        weights = [jnp.exp2(jnp.where(own, (row[:, pl.ds(128 * i, 128)] - high) * (head**-0.5 * LOG2E), -jnp.inf)) for i in range(rows // 128)]
        total = jnp.sum(tree(jnp.add, weights), -1, keepdims=True)
        weights = [jnp.concatenate([w.astype(jnp.bfloat16) for w in weights[i : i + 2]], -1) for i in range(0, len(weights), 2)]
        return weights, total, high

    def score(b, t):
        return lax.dot_general(q_ref[b], kbuf[lax.rem(b, SLOTS), pl.ds(256 * t, 256)], (((1,), (1,)), ((), ())), preferred_element_type=jnp.float32)

    def value(b, t, weights):
        return jnp.dot(weights[t], vbuf[lax.rem(b, SLOTS), pl.ds(256 * t, 256)], preferred_element_type=jnp.float32)

    def keep(b, found):
        for t, s in enumerate(found):
            scores[lax.rem(b, LEAD + 1), :, pl.ds(256 * t, 256)] = s

    def part(b, seen, total, high):
        parts[b, me] = seen.astype(jnp.bfloat16)
        row = jnp.where(lane == sublane, high * head**-0.5, 0.0) + jnp.where(lane == sublane + heads, total, 0.0)
        stats[b, me] = jnp.sum(row, 0, keepdims=True)

    def turn(b):
        weights, total, high = scale_rows(b - LEAD)
        found, seen = [], []
        for t in range(tiles + LAG):
            if t < tiles:
                found.append(score(b, t))
            if t >= LAG:
                seen.append(value(b - LEAD, t - LAG, weights))
        keep(b, found)
        part(b - LEAD, functools.reduce(jnp.add, seen), total, high)

    def values(b, weights):
        seen = [value(b, t, weights) for t in range(tiles)]
        one, other = functools.reduce(jnp.add, seen[::2]), functools.reduce(jnp.add, seen[1::2])
        return one + jnp.where(me >= 0, other, 0.0)

    def gather(b, sem):
        some = pl.ds(0, n - 1)
        remote(parts.at[b, some], psend, precv.at[sem], me).wait_recv()
        remote(stats.at[b, some], ssend, srecv.at[sem], me).wait_recv()
        high, total = [], []
        for i in range(n):
            row = jnp.broadcast_to(stats[b, i], (heads, 128))
            high.append(jnp.sum(jnp.where(lane == sublane, row, 0.0), -1, keepdims=True))
            total.append(jnp.sum(jnp.where(lane == sublane + heads, row, 0.0), -1, keepdims=True))
        top = tree(jnp.maximum, high)
        scale = [jnp.exp(h - top) for h in high]
        total = tree(jnp.add, [t * s for t, s in zip(total, scale)])
        seen = tree(jnp.add, [parts[b, i].astype(jnp.float32) * s for i, s in enumerate(scale)])
        done[b] = (seen / total).astype(jnp.bfloat16)

    def send(b):
        owner = lax.rem(b, n)

        @pl.when(me != owner)
        def _():
            send_part(b, b // n, owner)

    def own_up(b):
        @pl.when(me == lax.rem(b, n))
        def _():
            gather(b, b // n)
            for peer in peers:
                remote(done.at[b], dsend, drecv, peer).start()

    def send_all(b, some=slice(None)):
        for peer in peers[some]:
            send_part(b, b - shared + pl.cdiv(shared, n), peer)

    qcopy = pltpu.make_async_copy(q_hbm, q_ref, qsem)
    qcopy.start()
    for b in range(SLOTS):
        kcopy(b).start()
        if b >= LEAD:
            vcopy(b - LEAD).start()

    barrier = pltpu.get_barrier_semaphore()
    for peer in peers:
        pl.semaphore_signal(barrier, 1, device_id={"sp": peer}, device_id_type=pl.DeviceIdType.MESH)
    pl.semaphore_wait(barrier, n - 1)

    qcopy.wait()
    for b in range(LEAD):
        kcopy(b).wait()
        keep(b, [score(b, t) for t in range(tiles)])
        kcopy(b + SLOTS).start()
        vcopy(b + SLOTS - LEAD).start()

    def body(b, _):
        @pl.when((b > LEAD) & (b - LEAD - 1 < shared))
        def _():
            send(b - LEAD - 1)

        @pl.when(b - LEAD - 1 >= shared)
        def _():
            send_all(b - LEAD - 1)

        @pl.when((b >= WAIT) & (b - WAIT < shared))
        def _():
            own_up(b - WAIT)

        kcopy(b).wait()
        vcopy(b - LEAD).wait()
        turn(b)

        @pl.when(b + SLOTS < batch)
        def _():
            kcopy(b + SLOTS).start()

        @pl.when(b + SLOTS - LEAD < batch)
        def _():
            vcopy(b + SLOTS - LEAD).start()

    lax.fori_loop(LEAD, batch, body, None)
    ready = scale_rows(batch - LEAD)
    for b in range(batch - LEAD, batch):
        send_all(b - 1, slice(2))
        vcopy(b).wait()
        weights, total, high = ready
        if b + 1 < batch:
            ready = scale_rows(b + 1)
        part(b, values(b, weights), total, high)
    send_all(batch - 1)
    for b in range(batch - 2, batch - LEAD - 2, -1):
        send_all(b, slice(2, None))
    for b in range(batch - WAIT, shared):
        own_up(b)

    def last(b, _):
        gather(b, b - shared + pl.cdiv(shared, n))

    lax.fori_loop(shared, batch, last, None)

    for mine in {shared // n, pl.cdiv(shared, n)}:
        sent = shared - mine

        @pl.when((me < shared % n) == (mine > shared // n))
        def _():
            remote(done.at[pl.ds(0, sent)], dsend, drecv, me).wait_recv()
            for _ in range(mine):
                remote(done.at[pl.ds(0, n - 1)], dsend, drecv, me).wait_send()
            remote(parts.at[pl.ds(0, sent), 0], psend, precv.at[0], me).wait_send()
            remote(stats.at[pl.ds(0, sent), 0], ssend, srecv.at[0], me).wait_send()

    remote(parts.at[pl.ds(0, TAIL), pl.ds(0, n - 1)], psend, precv.at[0], me).wait_send()
    remote(stats.at[pl.ds(0, TAIL), pl.ds(0, n - 1)], ssend, srecv.at[0], me).wait_send()


def solution(mesh):
    n = mesh.shape["sp"]

    def step(q, k, v):
        batch, tokens, heads, head = k.shape
        rows = tokens * heads
        return pl.pallas_call(
            functools.partial(attend, n),
            out_shape=jax.ShapeDtypeStruct(q.shape, q.dtype),
            in_specs=[pl.BlockSpec(memory_space=pl.ANY)] * 3,
            out_specs=pl.BlockSpec(memory_space=pltpu.VMEM),
            scratch_shapes=[
                pltpu.VMEM((batch, heads, head), jnp.bfloat16),
                pltpu.VMEM((SLOTS, rows, head), jnp.bfloat16),
                pltpu.VMEM((SLOTS, rows, head), jnp.bfloat16),
                pltpu.VMEM((LEAD + 1, heads, rows), jnp.float32),
                pltpu.VMEM((batch, n, heads, head), jnp.bfloat16),
                pltpu.VMEM((batch, n, 1, 128), jnp.float32),
                pltpu.SemaphoreType.DMA,
                pltpu.SemaphoreType.DMA((SLOTS,)),
                pltpu.SemaphoreType.DMA((SLOTS,)),
                *[pltpu.SemaphoreType.DMA] * 4,
                *[pltpu.SemaphoreType.DMA((pl.cdiv(batch - TAIL, n) + TAIL,))] * 2,
            ],
            compiler_params=pltpu.CompilerParams(vmem_limit_bytes=215 * 2**18, collective_id=0, has_side_effects=True),
        )(q, k.reshape(batch, rows, head), v.reshape(batch, rows, head))

    return jax.shard_map(
        step,
        mesh=mesh,
        in_specs=(P("dp", None, None), P("dp", "sp", None, None), P("dp", "sp", None, None)),
        out_specs=P("dp", None, None),
        check_vma=False,
    )
```
